32 devices in a mesh: parts: 2 (over y), section: 2 (over core), tp: 8 (over z, x).
Axes of the slice: x: 2, y: 2, z: 4, core: 2. Of those that a mesh axis runs over, the one named last changes fastest.
Arguments:
- prompt_rows: bfloat16 [128, 8192], P(('parts', 'section', 'tp')), parts along dimension 0, may hold values from -72 to 72
- query_weight: bfloat16 [8192, 8192], P(None, 'tp'), may hold values from -0.0625 to 0.0625
- cache_weight: bfloat16 [8, 8192, 256], P('tp'), may hold values from -1 to 1, as said below
- output_weight: bfloat16 [8192, 8192], P('tp'), may hold values from -0.0625 to 0.0625
- documents: int32 [128], P('parts'), parts along dimension 0, may hold values from 0 to 3, never falling along the last dimension, each value on 1 to 32 neighbouring positions
- page_table: int32 [24], P('parts'), parts along dimension 0, may hold values from 0 to 15, as said below
Outputs:
- branch_output: bfloat16 [128, 8192], P(('parts', 'section', 'tp')), parts along dimension 0
- page_pool: bfloat16 [32, 8, 2048], P(('parts', 'section', 'tp')), parts along dimension 0
The draws below stay inside these ranges and needn't reach their ends.
There are 2 independent parts, one for each index of `parts`. The reference program is written for one: setup_inputs(seed, part) draws one part's arguments, and reference() takes and returns one part's arrays. A program takes and returns all parts, laid end to end along the dimension named above; an argument that names none is the same for every part. Nothing has to cross between parts.
Inputs may be any that keep to these rules, and one draw needn't show every extreme that they name: `cache_weight`: entry t equals entry u whenever t == u. `documents`: ids never fall along the tokens; there are 4 prompts of 1 to 32 tokens, one of exactly 32. `page_table`: entries are distinct pool slots; slot q is owned by the device of index q along section+tp (one slot per device). Entries beyond the number of pages are not used.
All inputs are finite; a program needn't handle non-finite values.
Results may differ from the reference program's by a relative error of at most 0.0085.
The reference program's roundings to bfloat16 on the way (of `queries`, `weights` and `attention`) count: a program that leaves them out, or rounds other values in their place, can miss the bound.
Values may be sent and summed in bfloat16 or wider, within the bound.
No kernel may reach another device: no remote copies, remote signals or barrier semaphores. Data moves between devices by JAX's collectives and lax.ppermute only.
A program may use at most 64 MiB of HBM per device.

```python
import math
import jax
import jax.numpy as jnp
import numpy as np
from jax import lax

D = 8192
HEADS = 64
KV_HEADS = 8
HEAD = 128
PAGE = 8
TOKENS = 64
DOCS = 4
LONGEST = 32
MAXP = 12
POOL = 16
N_TP = 8


def draw_prompt_rows(key, part):
    first_key = jax.random.fold_in(key, 11)
    values = jnp.clip(jax.random.normal(first_key, (TOKENS, D), jnp.float32), -6.0, 6.0)
    return values.astype(jnp.bfloat16)


def draw_cache_weight(key, part):
    base_key = jax.random.fold_in(key, 21)
    base = jnp.clip(jax.random.normal(base_key, (KV_HEADS, D, 2 * HEAD), jnp.float32), -6.0, 6.0)
    base = (base / jnp.sqrt(jnp.float32(D))).astype(jnp.bfloat16)
    return jnp.repeat(base, N_TP // KV_HEADS, axis=0)


def draw_page_table(key, part):
    table_key = jax.random.fold_in(key, 31)
    return jax.random.permutation(table_key, POOL)[:MAXP].astype(jnp.int32)


def level_of(stream_key, dims, cuts, smallest, high):
    def one(axis_at, parts):
        heights = jax.random.uniform(jax.random.fold_in(jax.random.fold_in(stream_key, 6), axis_at), (parts,), jnp.float32, smallest / len(cuts), high / len(cuts))
        return jnp.repeat(jnp.exp(heights), dims[axis_at] // parts).reshape((-1,) + (1,) * (len(dims) - axis_at - 1))

    level = one(*cuts[0])
    for cut in cuts[1:]:
        level = level * one(*cut)
    return level


def split_up(amount, total, most, skew):
    weights = [(1 << 20) // math.isqrt(rank ** skew) + 1 for rank in range(2, amount + 1)]
    surplus, holding = total - most - (amount - 1), [1] * (amount - 1)
    while surplus > 0:
        free = [i for i in range(amount - 1) if holding[i] < most]
        whole, budget = sum([weights[i] for i in free]), surplus
        for i in free:
            more = min(most - holding[i], max(1, budget * weights[i] // whole), surplus)
            holding[i] = holding[i] + more
            surplus = surplus - more
    return np.array([most] + holding)


def uneven_parts(key, amount, total, most, slope):
    if amount == 2:
        one = jax.random.randint(key, (), max(1, total - most), min(most, total - 1) + 1)
        return jnp.stack([one, total - one])
    tallies = jnp.asarray(split_up(amount, total, most, slope), jnp.int32)
    pairs = (amount - 1) // 2
    donor, taker = tallies[1:1 + 2 * pairs:2], tallies[2:2 + 2 * pairs:2]
    margin = jnp.minimum(donor - 1, most - taker)
    shifted = jax.random.randint(jax.random.fold_in(key, 1), (pairs,), 0, 1 << 20) % (margin + 1)
    tallies = tallies.at[1:1 + 2 * pairs:2].set(donor - shifted).at[2:2 + 2 * pairs:2].set(taker + shifted)
    return tallies[jax.random.permutation(jax.random.fold_in(key, 2), amount)]


def centred(stream_key, extent, scale, bound, pieces=(), kind=jnp.bfloat16):
    array = jax.random.normal(stream_key, extent, jnp.float32) * scale
    if len(pieces) > 0:
        array = level_of(stream_key, extent, pieces, -0.22, 0.18) * array
    return jnp.clip(array, min=-bound, max=bound).astype(kind)


def setup_inputs(seed: int = 0, part: int = 0) -> dict:
    seeds = jax.random.split(jax.random.key(seed), 7)
    own_keys = jax.random.split(jax.random.fold_in(seeds[6], part), 7)
    return {
        "prompt_rows": draw_prompt_rows(jax.random.fold_in(jax.random.fold_in(seeds[6], part), 71), part),
        "query_weight": centred(seeds[1], (D, HEADS * HEAD), D ** -0.5, 0.0625, ((1, 8),)),
        "cache_weight": draw_cache_weight(jax.random.fold_in(seeds[6], 71), part),
        "output_weight": centred(seeds[3], (HEADS * HEAD, D), (HEADS * HEAD) ** -0.5, 0.0625, ((0, 8),)),
        "documents": jnp.searchsorted(jnp.cumsum(uneven_parts(own_keys[4], DOCS, TOKENS, LONGEST, 2)), jnp.arange(TOKENS), side="right").astype(jnp.int32),
        "page_table": draw_page_table(jax.random.fold_in(jax.random.fold_in(seeds[6], part), 71), part),
    }


rope_base = 500000.0


def document_layout(documents):
    count = documents.shape[0]
    places = jnp.arange(count, dtype=jnp.int32)
    begins = jnp.concatenate([jnp.ones((1,), dtype=bool), documents[1:] != documents[:-1]])
    firsts = lax.cummax(jnp.where(begins, places, jnp.zeros_like(places)), axis=0)
    offsets = (places - firsts).astype(jnp.int32)
    starts = (offsets % PAGE == 0).astype(jnp.int32)
    pages = (jnp.cumsum(starts) - 1).astype(jnp.int32)
    return offsets, pages


def rope_tables(offsets, width):
    half_width = width // 2
    freqs = rope_base ** (-(jnp.arange(half_width, dtype=jnp.float32) * 2.0 / width))
    angles = offsets.astype(jnp.float32)[:, None] * freqs[None, :]
    return jnp.cos(angles), jnp.sin(angles)


def rotate(values, cosines, sines):
    half_width = values.shape[-1] // 2
    first = values[..., :half_width]
    second = values[..., half_width:]
    return jnp.concatenate([first * cosines - second * sines, second * cosines + first * sines], axis=-1)


def reference(prompt_rows, query_weight, cache_weight, output_weight, documents, page_table):
    offsets, pages = document_layout(documents)
    cosines, sines = rope_tables(offsets, HEAD)
    queries = jnp.dot(prompt_rows, query_weight, preferred_element_type=jnp.float32)
    queries = queries.reshape(TOKENS, HEADS, HEAD)
    queries = rotate(queries, cosines[:, None, :], sines[:, None, :]).astype(jnp.bfloat16)
    copies = N_TP // KV_HEADS
    heads_weight = cache_weight[::copies]
    flat_weight = jnp.transpose(heads_weight, (1, 0, 2)).reshape(D, KV_HEADS * 2 * HEAD)
    keyvals = jnp.dot(prompt_rows, flat_weight, preferred_element_type=jnp.float32)
    keyvals = keyvals.reshape(TOKENS, KV_HEADS, 2 * HEAD)
    keys = rotate(keyvals[..., :HEAD], cosines[:, None, :], sines[:, None, :]).astype(jnp.bfloat16)
    values = keyvals[..., HEAD:].astype(jnp.bfloat16)
    places = jnp.arange(TOKENS, dtype=jnp.int32)
    allowed = (documents[:, None] == documents[None, :]) & (places[None, :] <= places[:, None])
    scale = 1.0 / (HEAD ** 0.5)
    group_size = HEADS // KV_HEADS

    def one_head(index):
        query = lax.dynamic_index_in_dim(queries, index, 1, keepdims=False)
        group = index // group_size
        key = lax.dynamic_index_in_dim(keys, group, 1, keepdims=False)
        value = lax.dynamic_index_in_dim(values, group, 1, keepdims=False)
        scores = jnp.dot(query, key.T, preferred_element_type=jnp.float32) * scale
        scores = jnp.where(allowed, scores, -jnp.inf)
        weights = jax.nn.softmax(scores, axis=-1).astype(jnp.bfloat16)
        return jnp.dot(weights, value, preferred_element_type=jnp.float32).astype(jnp.bfloat16)

    heads_out = lax.map(one_head, jnp.arange(HEADS, dtype=jnp.int32))
    attention = jnp.transpose(heads_out, (1, 0, 2)).reshape(TOKENS, HEADS * HEAD)
    branch_output = jnp.dot(attention, output_weight, preferred_element_type=jnp.float32).astype(jnp.bfloat16)
    cache_rows = jnp.concatenate([keys.reshape(TOKENS, KV_HEADS * HEAD), values.reshape(TOKENS, KV_HEADS * HEAD)], axis=1)
    row_of = (page_table[pages] * PAGE + offsets % PAGE).astype(jnp.int32)
    pool = jnp.zeros((POOL * PAGE, 2 * KV_HEADS * HEAD), jnp.bfloat16).at[row_of].set(cache_rows)
    return branch_output, pool.reshape(POOL, PAGE, 2 * KV_HEADS * HEAD)
```

```python
import jax
import jax.numpy as jnp
from jax import lax
from jax.sharding import PartitionSpec as P

KV_HEADS = 8
HEAD = 128
PAGE = 8
FEW = 8


rope_base = 500000.0


def from_partner(value, axis, mask):
    pairs = [(source, source ^ mask) for source in range(lax.axis_size(axis))]
    return lax.ppermute(value, axis, pairs)


def few_devices(count):
    return 4 <= count <= FEW and count & (count - 1) == 0


def gather_rows(rows):
    count = lax.axis_size("tp")
    if not few_devices(count):
        return lax.all_gather(rows, "tp", axis=0, tiled=True)
    column = lax.axis_index("tp")
    blocks = {0: rows}
    for mask in range(2, count, 2):
        blocks[mask] = from_partner(rows, "tp", mask)
    for mask in range(0, count, 2):
        blocks[mask + 1] = from_partner(blocks[mask], "tp", 1)
    stacked = jnp.stack([blocks[mask] for mask in range(count)], axis=0)
    pieces = []
    for place in range(count):
        piece = lax.dynamic_index_in_dim(stacked, place ^ column, 0, keepdims=False)
        pieces.append(piece)
    return jnp.concatenate(pieces, axis=0)


def scatter_sum(partial, rows_dev):
    count = lax.axis_size("tp")
    if not few_devices(count):
        return lax.psum_scatter(partial, "tp", scatter_dimension=0, tiled=True)
    column = lax.axis_index("tp")
    blocks = partial.reshape(count, rows_dev, partial.shape[1])
    total = lax.dynamic_index_in_dim(blocks, column, 0, keepdims=False)
    narrow = blocks.astype(jnp.bfloat16)
    for mask in range(count - 1, 0, -1):
        sent = lax.dynamic_index_in_dim(narrow, column ^ mask, 0, keepdims=False)
        total = total + from_partner(sent, "tp", mask).astype(jnp.float32)
    return total


def document_layout(documents):
    count = documents.shape[0]
    places = jnp.arange(count, dtype=jnp.int32)
    firsts = jnp.sum((documents[None, :] < documents[:, None]).astype(jnp.int32), axis=1)
    offsets = places - firsts
    starts = (offsets % PAGE == 0)[None, :] & (places[None, :] <= places[:, None])
    pages = jnp.sum(starts.astype(jnp.int32), axis=1) - 1
    return (offsets, pages)


def rope_tables(offsets, width):
    half_width = width // 2
    freqs = rope_base ** (-(jnp.arange(half_width, dtype=jnp.float32) * 2.0 / width))
    angles = offsets.astype(jnp.float32)[:, None] * freqs[None, :]
    return (jnp.cos(angles), jnp.sin(angles))


def rotate(values, cosines, sines):
    half_width = values.shape[-1] // 2
    first = values[..., :half_width]
    second = values[..., half_width:]
    return jnp.concatenate(
        [first * cosines - second * sines, second * cosines + first * sines], axis=-1
    )


def finish_cache(keyvals, cosines, sines):
    rotated = rotate(keyvals[:, :HEAD], cosines, sines)
    return jnp.concatenate([rotated, keyvals[:, HEAD:]], axis=1).astype(jnp.bfloat16)


def body(prompt_rows, query_weight, cache_weight, output_weight, documents, page_table):
    tp_count = lax.axis_size("tp")
    owners = lax.axis_size(("section", "tp"))
    section = lax.axis_index("section")
    column = lax.axis_index("tp")
    rows_dev = prompt_rows.shape[0]
    half_rows = rows_dev * tp_count
    total_rows = 2 * half_rows
    query_width = query_weight.shape[1]
    query_heads = query_width // HEAD
    replicas = tp_count // KV_HEADS
    slice_width = HEAD // replicas
    head_weight = cache_weight[0]
    offsets, pages = document_layout(documents)
    cosines, sines = rope_tables(offsets, HEAD)
    own_start = section * half_rows
    own_cos = lax.dynamic_slice_in_dim(cosines, own_start, half_rows, 0)
    own_sin = lax.dynamic_slice_in_dim(sines, own_start, half_rows, 0)
    piece = gather_rows(prompt_rows)
    cache_rows = jnp.dot(piece, head_weight, preferred_element_type=jnp.float32)
    query_part = jnp.dot(piece, query_weight, preferred_element_type=jnp.float32)
    cache_half = finish_cache(cache_rows, own_cos, own_sin)
    other = from_partner(cache_half, "section", 1)
    lower = jnp.where(section == 0, cache_half, other)
    upper = jnp.where(section == 0, other, cache_half)
    cache_all = jnp.concatenate([lower, upper], axis=0)
    queries = query_part.reshape(half_rows, query_heads, HEAD)
    queries = rotate(queries, own_cos[:, None, :], own_sin[:, None, :]).astype(jnp.bfloat16)
    keys = cache_all[:, :HEAD]
    values = cache_all[:, HEAD:]
    places = jnp.arange(total_rows, dtype=jnp.int32)
    query_places = own_start + jnp.arange(half_rows, dtype=jnp.int32)
    query_docs = lax.dynamic_slice_in_dim(documents, own_start, half_rows, 0)
    allowed = (query_docs[:, None] == documents[None, :]) & (
        places[None, :] <= query_places[:, None]
    )
    scale = 1.0 / HEAD**0.5
    scores = jnp.einsum("qhd,kd->hqk", queries, keys, preferred_element_type=jnp.float32) * scale
    scores = jnp.where(allowed[None, :, :], scores, -jnp.inf)
    weights = jax.nn.softmax(scores, axis=-1).astype(jnp.bfloat16)
    mixed = jnp.einsum("hqk,kd->qhd", weights, values, preferred_element_type=jnp.float32)
    attention = mixed.astype(jnp.bfloat16).reshape(half_rows, query_heads * HEAD)
    column_start = section * HEAD + column % replicas * slice_width
    share = lax.dynamic_slice_in_dim(cache_all, column_start, slice_width, 1)
    capacity = rows_dev // 4 * PAGE
    slots = jnp.arange(page_table.shape[0], dtype=jnp.int32)
    hit = pages[:, None] == slots[None, :]
    table_at = jnp.sum(jnp.where(hit, page_table[None, :], 0), axis=1)
    row_of = table_at * PAGE + offsets % PAGE
    pool_rows = jnp.arange(owners * capacity, dtype=jnp.int32)
    placed = (pool_rows[:, None] == row_of[None, :]).astype(jnp.bfloat16)
    outgoing = jnp.dot(placed, share, preferred_element_type=jnp.float32).astype(jnp.bfloat16)
    outgoing = outgoing.reshape(owners, capacity, slice_width)
    arrived = lax.all_to_all(outgoing, ("section", "tp"), split_axis=0, concat_axis=2, tiled=True)
    partial = jnp.dot(attention, output_weight, preferred_element_type=jnp.float32)
    branch_output = scatter_sum(partial, rows_dev).astype(jnp.bfloat16)
    return (branch_output, arrived)


def solution(mesh):
    return jax.shard_map(
        body,
        mesh=mesh,
        in_specs=(
            P(("parts", "section", "tp"), None),
            P(None, "tp"),
            P("tp", None, None),
            P("tp", None),
            P("parts"),
            P("parts"),
        ),
        out_specs=(P(("parts", "section", "tp"), None), P(("parts", "section", "tp"), None, None)),
        check_vma=False,
    )
```

```python
import functools

import jax
import jax.numpy as jnp
import numpy as np
from jax import lax
from jax.experimental import pallas as pl
from jax.experimental.pallas import tpu as pltpu
from jax.sharding import PartitionSpec as P

KV_HEADS = 8
HEAD = 128
PAGE = 8
FEW = 8
VM = pl.BlockSpec(memory_space=pltpu.VMEM)
SM = pl.BlockSpec(memory_space=pltpu.SMEM)
ANY = pl.BlockSpec(memory_space=pl.ANY)


rope_base = 500000.0


def from_partner(value, axis, mask):
    pairs = [(source, source ^ mask) for source in range(lax.axis_size(axis))]
    return lax.ppermute(value, axis, pairs)


def document_layout(documents):
    count = documents.shape[0]
    places = jnp.arange(count, dtype=jnp.int32)
    firsts = jnp.sum((documents[None, :] < documents[:, None]).astype(jnp.int32), axis=1)
    offsets = places - firsts
    starts = (offsets % PAGE == 0)[None, :] & (places[None, :] <= places[:, None])
    pages = jnp.sum(starts.astype(jnp.int32), axis=1) - 1
    return (offsets, pages)


def rope_tables(offsets, width):
    half_width = width // 2
    freqs = rope_base ** (-(jnp.arange(half_width, dtype=jnp.float32) * 2.0 / width))
    angles = offsets.astype(jnp.float32)[:, None] * freqs[None, :]
    return (jnp.cos(angles), jnp.sin(angles))


def rotate(values, cosines, sines):
    half_width = values.shape[-1] // 2
    first = values[..., :half_width]
    second = values[..., half_width:]
    return jnp.concatenate(
        [first * cosines - second * sines, second * cosines + first * sines], axis=-1
    )


def finish_cache(keyvals, cosines, sines):
    rotated = rotate(keyvals[:, :HEAD], cosines, sines)
    return jnp.concatenate([rotated, keyvals[:, HEAD:]], axis=1).astype(jnp.bfloat16)


def body_many(prompt_rows, query_weight, cache_weight, output_weight, documents, page_table):
    tp_count = lax.axis_size("tp")
    owners = lax.axis_size(("section", "tp"))
    section = lax.axis_index("section")
    column = lax.axis_index("tp")
    rows_dev = prompt_rows.shape[0]
    half_rows = rows_dev * tp_count
    total_rows = 2 * half_rows
    query_width = query_weight.shape[1]
    query_heads = query_width // HEAD
    replicas = tp_count // KV_HEADS
    slice_width = HEAD // replicas
    head_weight = cache_weight[0]
    offsets, pages = document_layout(documents)
    cosines, sines = rope_tables(offsets, HEAD)
    own_start = section * half_rows
    own_cos = lax.dynamic_slice_in_dim(cosines, own_start, half_rows, 0)
    own_sin = lax.dynamic_slice_in_dim(sines, own_start, half_rows, 0)
    piece = lax.all_gather(prompt_rows, "tp", axis=0, tiled=True)
    cache_rows = jnp.dot(piece, head_weight, preferred_element_type=jnp.float32)
    query_part = jnp.dot(piece, query_weight, preferred_element_type=jnp.float32)
    cache_half = finish_cache(cache_rows, own_cos, own_sin)
    other = from_partner(cache_half, "section", 1)
    lower = jnp.where(section == 0, cache_half, other)
    upper = jnp.where(section == 0, other, cache_half)
    cache_all = jnp.concatenate([lower, upper], axis=0)
    queries = query_part.reshape(half_rows, query_heads, HEAD)
    queries = rotate(queries, own_cos[:, None, :], own_sin[:, None, :]).astype(jnp.bfloat16)
    keys = cache_all[:, :HEAD]
    values = cache_all[:, HEAD:]
    places = jnp.arange(total_rows, dtype=jnp.int32)
    query_places = own_start + jnp.arange(half_rows, dtype=jnp.int32)
    query_docs = lax.dynamic_slice_in_dim(documents, own_start, half_rows, 0)
    allowed = (query_docs[:, None] == documents[None, :]) & (
        places[None, :] <= query_places[:, None]
    )
    scale = 1.0 / HEAD**0.5
    scores = jnp.einsum("qhd,kd->hqk", queries, keys, preferred_element_type=jnp.float32) * scale
    scores = jnp.where(allowed[None, :, :], scores, -jnp.inf)
    weights = jax.nn.softmax(scores, axis=-1).astype(jnp.bfloat16)
    mixed = jnp.einsum("hqk,kd->qhd", weights, values, preferred_element_type=jnp.float32)
    attention = mixed.astype(jnp.bfloat16).reshape(half_rows, query_heads * HEAD)
    column_start = section * HEAD + column % replicas * slice_width
    share = lax.dynamic_slice_in_dim(cache_all, column_start, slice_width, 1)
    capacity = rows_dev // 4 * PAGE
    slots = jnp.arange(page_table.shape[0], dtype=jnp.int32)
    hit = pages[:, None] == slots[None, :]
    table_at = jnp.sum(jnp.where(hit, page_table[None, :], 0), axis=1)
    row_of = table_at * PAGE + offsets % PAGE
    pool_rows = jnp.arange(owners * capacity, dtype=jnp.int32)
    placed = (pool_rows[:, None] == row_of[None, :]).astype(jnp.bfloat16)
    outgoing = jnp.dot(placed, share, preferred_element_type=jnp.float32).astype(jnp.bfloat16)
    outgoing = outgoing.reshape(owners, capacity, slice_width)
    arrived = lax.all_to_all(outgoing, ("section", "tp"), split_axis=0, concat_axis=2, tiled=True)
    partial = jnp.dot(attention, output_weight, preferred_element_type=jnp.float32)
    summed = lax.psum_scatter(partial, "tp", scatter_dimension=0, tiled=True)
    return (summed.astype(jnp.bfloat16), arrived)


def stream(count, rows, source, target, sems):
    return [
        pltpu.make_async_copy(
            source.at[pl.ds(i * rows, rows), :], target.at[pl.ds(i * rows, rows), :], sems.at[i]
        )
        for i in range(count)
    ]


def layout_kernel(
    rows_dev, capacity, place_ref, docs_ref, table_ref, freq_ref, cos_ref, sin_ref, allow_ref, put_ref
):
    section, column = place_ref[0], place_ref[1]
    total = docs_ref.shape[1]
    half = total // 2
    i32 = jnp.int32
    sub = lax.broadcasted_iota(i32, (total, total), 0)
    lane = lax.broadcasted_iota(i32, (total, total), 1)
    eye = sub == lane

    def token_of(place):
        within = place % half
        return place // half * half + (within // rows_dev ^ column) * rows_dev + within % rows_dev

    def to_column(row):
        return jnp.sum(jnp.where(eye, row, 0), axis=1, keepdims=True)

    def to_row(col):
        return jnp.sum(jnp.where(eye, col, 0), axis=0, keepdims=True)

    doc_row = docs_ref[...]
    doc_col = to_column(doc_row)
    first = jnp.sum((doc_row < doc_col).astype(i32), axis=1, keepdims=True)
    token_col = lax.broadcasted_iota(i32, (total, 1), 0)
    off_col = token_col - first
    off_row = to_row(off_col)
    begins = (off_row % PAGE == 0) & (lane <= sub)
    page_col = jnp.sum(begins.astype(i32), axis=1, keepdims=True) - 1
    slots = lax.broadcasted_iota(i32, (total, table_ref.shape[1]), 1)
    slot_col = jnp.sum(jnp.where(slots == page_col, table_ref[...], 0), axis=1, keepdims=True)
    row_col = slot_col * PAGE + off_col % PAGE
    by_place = lane == token_of(sub)
    place_off = jnp.sum(jnp.where(by_place, off_row, 0), axis=1, keepdims=True)
    place_doc = jnp.sum(jnp.where(by_place, doc_row, 0), axis=1, keepdims=True)
    to_place = sub == token_of(lane)
    place_doc_row = jnp.sum(jnp.where(to_place, doc_col, 0), axis=0, keepdims=True)
    place_row_row = jnp.sum(jnp.where(to_place, row_col, 0), axis=0, keepdims=True)
    upper = section == 1
    own_doc = jnp.where(upper, place_doc[half:], place_doc[:half])
    own_off = jnp.where(upper, place_off[half:], place_off[:half])
    own_token = token_of(section * half + lax.broadcasted_iota(i32, (half, total), 0))
    key_token = token_of(lax.broadcasted_iota(i32, (half, total), 1))
    allow = (own_doc == place_doc_row) & (key_token <= own_token)
    allow_ref[...] = allow.astype(jnp.float32)
    angle = own_off.astype(jnp.float32) * freq_ref[...]
    cos_ref[...] = jnp.cos(angle)
    lanes = lax.broadcasted_iota(i32, angle.shape, 1)
    sines = jnp.sin(angle)
    sin_ref[...] = jnp.where(lanes < HEAD // 2, -sines, sines)
    tp_count = half // rows_dev
    out_rows = tp_count * capacity
    out_sub = lax.broadcasted_iota(i32, (out_rows, total), 0)
    owner = section * tp_count + (out_sub // capacity ^ column)
    wanted = owner * capacity + out_sub % capacity
    put_ref[...] = (wanted == place_row_row).astype(jnp.bfloat16)


def turn(values, cosines, sines):
    return values * cosines + pltpu.roll(values, HEAD // 2, 1) * sines


def cache_kernel(
    count, *refs
):
    blocks, (weight, cos_ref, sin_ref, rows_ref, cache_ref, held, sems) = refs[:count], refs[count:]
    depth = weight.shape[0]
    chunks = sems.shape[0]
    step = depth // chunks
    copies = stream(chunks, step, weight, held, sems)
    for copy in copies:
        copy.start()
    rows_dev = blocks[0].shape[0]
    pair = max(1, 8 // rows_dev)
    for m in range(0, count, pair):
        joined = jnp.concatenate([blocks[m + j][...].astype(jnp.float32) for j in range(pair)], axis=0)
        rows_ref[pl.ds(m * rows_dev, pair * rows_dev), :] = joined.astype(jnp.bfloat16)
    total = jnp.zeros(cache_ref.shape, jnp.float32)
    for i, copy in enumerate(copies):
        copy.wait()
        total += jnp.dot(
            rows_ref[:, i * step : (i + 1) * step],
            held[i * step : (i + 1) * step, :],
            preferred_element_type=jnp.float32,
        )
    cache_ref[:, :HEAD] = turn(total[:, :HEAD], cos_ref[...], sin_ref[...]).astype(jnp.bfloat16)
    cache_ref[:, HEAD:] = total[:, HEAD:].astype(jnp.bfloat16)


def query_kernel(rows_ref, weight, cos_ref, sin_ref, query_ref, held, sems):
    depth = weight.shape[0]
    chunks = sems.shape[0]
    step = depth // chunks
    copies = stream(chunks, step, weight, held, sems)
    for copy in copies:
        copy.start()
    total = jnp.zeros(query_ref.shape, jnp.float32)
    for i, copy in enumerate(copies):
        copy.wait()
        total += jnp.dot(
            rows_ref[:, i * step : (i + 1) * step],
            held[i * step : (i + 1) * step, :],
            preferred_element_type=jnp.float32,
        )
    for h in range(query_ref.shape[1] // HEAD):
        at = slice(h * HEAD, (h + 1) * HEAD)
        query_ref[:, at] = turn(total[:, at], cos_ref[...], sin_ref[...]).astype(jnp.bfloat16)


def output_kernel(
    count, place_ref, query_ref, own_ref, other_ref, allow_ref, put_ref, weight, *rest
):
    outs, own_out, own_cache, (held, sems) = rest[: count - 1], rest[count - 1], rest[count], rest[count + 1 :]
    chunks = sems.shape[0]
    width = weight.shape[1]
    step = width // chunks
    copies = [
        pltpu.make_async_copy(
            weight.at[:, pl.ds(i * step, step)], held.at[:, pl.ds(i * step, step)], sems.at[i]
        )
        for i in range(chunks)
    ]
    for copy in copies:
        copy.start()
    half = query_ref.shape[0]
    rows_dev = half // count
    heads = query_ref.shape[1] // HEAD
    first = place_ref[0] == 0
    own, other = own_ref[...], other_ref[...]
    cache = jnp.concatenate([jnp.where(first, own, other), jnp.where(first, other, own)], axis=0)
    keys, values = cache[:, :HEAD], cache[:, HEAD:]
    allow = allow_ref[...] > 0.5
    mixed = []
    for h in range(heads):
        query = query_ref[:, h * HEAD : (h + 1) * HEAD]
        scores = lax.dot_general(
            query, keys, (((1,), (1,)), ((), ())), preferred_element_type=jnp.float32
        )
        scores = jnp.where(allow, scores * (1.0 / HEAD**0.5), -jnp.inf)
        top = jnp.max(scores, axis=1, keepdims=True)
        raised = jnp.exp(scores - top)
        weights = (raised / jnp.sum(raised, axis=1, keepdims=True)).astype(jnp.bfloat16)
        mixed.append(jnp.dot(weights, values, preferred_element_type=jnp.float32).astype(jnp.bfloat16))
    attention = jnp.concatenate(mixed, axis=1)
    placed = jnp.dot(put_ref[...], cache, preferred_element_type=jnp.float32)
    capacity = put_ref.shape[0] // count
    wide = 2 * HEAD
    own_cache[...] = placed[:capacity].astype(jnp.bfloat16)
    for m in range(1, count):
        mine = placed[m * capacity : (m + 1) * capacity].astype(jnp.bfloat16)
        for part in range(capacity // rows_dev):
            outs[m - 1][:, width + part * wide : width + (part + 1) * wide] = mine[
                part * rows_dev : (part + 1) * rows_dev
            ]
    for i, copy in enumerate(copies):
        copy.wait()
        at = slice(i * step, (i + 1) * step)
        part = jnp.dot(attention, held[:, at], preferred_element_type=jnp.float32)
        own_out[:, at] = part[:rows_dev]
        for m in range(1, count):
            outs[m - 1][:, at] = part[m * rows_dev : (m + 1) * rows_dev].astype(jnp.bfloat16)


def finish_kernel(count, place_ref, *rest):
    got, (own_out, own_cache, branch_ref, pool_ref) = rest[: count - 1], rest[count - 1 :]
    column = place_ref[1]
    rows_dev, width = own_out.shape
    capacity = own_cache.shape[0]
    wide = 2 * HEAD
    total = own_out[...]
    for block in got:
        total += block[:, :width].astype(jnp.float32)
    branch_ref[...] = total.astype(jnp.bfloat16)
    for m in range(count):
        if m == 0:
            cache = own_cache[...]
        else:
            cache = jnp.concatenate(
                [
                    got[m - 1][:, width + part * wide : width + (part + 1) * wide].astype(jnp.float32)
                    for part in range(capacity // rows_dev)
                ],
                axis=0,
            ).astype(jnp.bfloat16)
        head = column ^ m
        pool_ref[0, :, pl.ds(pl.multiple_of(head * HEAD, HEAD), HEAD)] = cache[:, :HEAD]
        pool_ref[0, :, pl.ds(pl.multiple_of((count + head) * HEAD, HEAD), HEAD)] = cache[:, HEAD:]


def params(mib):
    return pltpu.CompilerParams(vmem_limit_bytes=mib << 20)


def cost(flops, read):
    return pl.CostEstimate(flops=flops, bytes_accessed=read, transcendentals=0)


def body_few(prompt_rows, query_weight, cache_weight, output_weight, documents, page_table):
    count = lax.axis_size("tp")
    section = lax.axis_index("section")
    column = lax.axis_index("tp")
    rows_dev, depth = prompt_rows.shape
    half = rows_dev * count
    total = 2 * half
    query_width = query_weight.shape[1]
    out_width = output_weight.shape[1]
    capacity = rows_dev // 4 * PAGE
    bf16, f32 = jnp.bfloat16, jnp.float32
    shape = jax.ShapeDtypeStruct
    place = jnp.stack([section, column]).astype(jnp.int32)
    bands = np.float64(rope_base) ** (-(np.arange(HEAD // 2) * 2.0 / HEAD))
    freqs = jnp.asarray(np.concatenate([bands, bands])[None, :], f32)

    blocks = {0: prompt_rows}
    for mask in range(2, count, 2):
        blocks[mask] = from_partner(prompt_rows, "tp", mask)
    for mask in range(0, count, 2):
        blocks[mask + 1] = from_partner(blocks[mask], "tp", 1)

    cosines, sines, allow, put = pl.pallas_call(
        functools.partial(layout_kernel, rows_dev, capacity),
        out_shape=(
            shape((half, HEAD), f32),
            shape((half, HEAD), f32),
            shape((half, total), f32),
            shape((count * capacity, total), bf16),
        ),
        in_specs=[SM, VM, VM, VM],
        out_specs=(VM, VM, VM, VM),
        compiler_params=params(4),
        name="layout",
    )(place, documents[None, :], page_table[None, :], freqs)

    rows, cache = pl.pallas_call(
        functools.partial(cache_kernel, count),
        out_shape=(shape((half, depth), bf16), shape((half, 2 * HEAD), bf16)),
        in_specs=[VM] * count + [ANY, VM, VM],
        out_specs=(VM, VM),
        scratch_shapes=[pltpu.VMEM((depth, 2 * HEAD), bf16), pltpu.SemaphoreType.DMA((4,))],
        compiler_params=params(8),
        cost_estimate=cost(2 * half * depth * 2 * HEAD, depth * 4 * HEAD),
        name="cache",
    )(*[blocks[m] for m in range(count)], cache_weight[0], cosines, sines)

    other = from_partner(cache, "section", 1)

    queries = pl.pallas_call(
        query_kernel,
        out_shape=shape((half, query_width), bf16),
        in_specs=[VM, ANY, VM, VM],
        out_specs=VM,
        scratch_shapes=[pltpu.VMEM((depth, query_width), bf16), pltpu.SemaphoreType.DMA((16,))],
        compiler_params=params(24),
        cost_estimate=cost(2 * half * depth * query_width, 2 * depth * query_width),
        name="query",
    )(rows, query_weight, cosines, sines)

    spare = capacity // rows_dev * 2 * HEAD
    sent = pl.pallas_call(
        functools.partial(output_kernel, count),
        out_shape=tuple(shape((rows_dev, out_width + spare), bf16) for _ in range(count - 1))
        + (shape((rows_dev, out_width), f32), shape((capacity, 2 * HEAD), bf16)),
        in_specs=[SM, VM, VM, VM, VM, VM, ANY],
        out_specs=(VM,) * (count + 1),
        scratch_shapes=[pltpu.VMEM((query_width, out_width), bf16), pltpu.SemaphoreType.DMA((16,))],
        compiler_params=params(24),
        cost_estimate=cost(2 * half * out_width * query_width, 2 * out_width * query_width),
        name="output",
    )(place, queries, cache, other, allow, put, output_weight)

    got = [None] * (count - 1)
    for mask in range(count - 1, 0, -1):
        got[mask - 1] = from_partner(sent[mask - 1], "tp", mask)

    branch, pool = pl.pallas_call(
        functools.partial(finish_kernel, count),
        out_shape=(shape((rows_dev, out_width), bf16), shape((1, capacity, 2 * count * HEAD), bf16)),
        in_specs=[SM] + [VM] * (count + 1),
        out_specs=(VM, VM),
        compiler_params=params(8),
        name="finish",
    )(place, *got, sent[count - 1], sent[count])
    return (branch, pool)


def solution(mesh):
    count = mesh.shape["tp"]
    few = count == KV_HEADS and count <= FEW and count & (count - 1) == 0
    return jax.shard_map(
        body_few if few else body_many,
        mesh=mesh,
        in_specs=(
            P(("parts", "section", "tp"), None),
            P(None, "tp"),
            P("tp", None, None),
            P("tp", None),
            P("parts"),
            P("parts"),
        ),
        out_specs=(P(("parts", "section", "tp"), None), P(("parts", "section", "tp"), None, None)),
        check_vma=False,
    )
```
